32 devices in a mesh: wide: 8 (over z, y), narrow: 4 (over x, core).
Axes of the slice: x: 2, y: 2, z: 4, core: 2. Of those that a mesh axis runs over, the one named last changes fastest.
Arguments:
- noise: bfloat16 [128, 32, 256], P('wide'), may hold values from -6 to 6
- diagonal_tile_blocks: bfloat16 [128, 256, 256], P(('wide', 'narrow')), may hold values from -0.375 to 0.375
- left_factors: bfloat16 [128, 128, 128, 256], P('wide', 'narrow'), may hold values from -0.046875 to 0.046875
- right_factors: bfloat16 [128, 128, 128, 256], P('wide', 'narrow'), may hold values from -0.375 to 0.375
- ranks: int32 [128, 128], P('wide', 'narrow'), may hold values from 0 to 128, as said below
- owner: int32 [128], replicated, may hold values from 0 to 127, as said below
- courant_x: float32 [128, 256], P('wide', 'narrow'), may hold values from 0.05 to 0.4
- courant_number_second: float32 [128, 256], P('wide', 'narrow'), may hold values from 0.05 to 0.4
- upwind_x: int32 [128, 256], P('wide', 'narrow'), may hold values from 0 to 1
- upwind_y: int32 [128, 256], P('wide', 'narrow'), may hold values from 0 to 1
Outputs:
- tracer: float32 [32, 128, 256], P(None, 'wide', 'narrow')
The draws below stay inside these ranges and needn't reach their ends.
Inputs may be any that keep to these rules, and one draw needn't show every extreme that they name: owner is a permutation of the tile rows 0 to 127. ranks[p, c] is 0 where c >= owner[p] and at least 1 where c < owner[p].
All inputs are finite; a program needn't handle non-finite values.
Results may differ from the reference program's by a relative error of at most 0.0016.
Values may be sent and summed in bfloat16 or wider, within the bound.
A program may use at most 128 MiB of HBM per device.

```python
import jax
import jax.numpy as jnp
import numpy as np
from jax import lax

TSIDE = 16
R = 128
S = 32
TX = 8
TY = 16
ITERS = 4
TS = 256
NT = 128
GX = 128
GY = 256


def owner_of(key):
    return jax.random.permutation(jax.random.fold_in(key, 11), NT).astype(jnp.int32)


def draw_owner(key, part):
    return owner_of(key)


def draw_ranks(key, part):
    holder = owner_of(key)
    tile_rows = holder[:, None]
    tile_cols = jnp.arange(NT, dtype=jnp.int32)[None, :]
    raw_ranks = jax.random.randint(jax.random.fold_in(key, 12), (NT, NT), 1, R + 1).astype(jnp.int32)
    forced = (tile_rows == NT - 1) & (tile_cols == 0)
    raw_ranks = jnp.where(forced, R, raw_ranks)
    return jnp.where(tile_cols < tile_rows, raw_ranks, 0).astype(jnp.int32)


def place_ends(drawn, own_key, low, top_value):
    dims = drawn.shape
    index_at = [jax.random.randint(jax.random.fold_in(own_key, axis), (), 0, dims[axis]) for axis in range(len(dims))]
    drawn = drawn.at[tuple(index_at)].set(low)
    longest = dims.index(max(dims))
    index_at[longest] = (index_at[longest] + 1) % dims[longest]
    return drawn.at[tuple(index_at)].set(top_value)


def block_scale(key, dims, split, least, top_value):
    loudness = 1.0
    for dim, parts in split:
        heights = jax.random.uniform(jax.random.fold_in(jax.random.fold_in(key, 6), dim), (parts,), jnp.float32, least / len(split), top_value / len(split))
        loudness = loudness * jnp.repeat(jnp.exp(heights), dims[dim] // parts).reshape((-1,) + (1,) * (len(dims) - 1 - dim))
    return loudness


def gaussian(stream_key, extent, spread, limit, split=(), kind=jnp.bfloat16):
    loudness = block_scale(stream_key, extent, split, -0.22, 0.18) if split else 1.0
    result = jax.random.normal(stream_key, extent, jnp.float32) * spread * loudness
    return jnp.minimum(jnp.maximum(result, -limit), limit).astype(kind)


def setup_inputs(seed: int = 0) -> dict:
    splits = jax.random.split(jax.random.key(seed), 11)
    return {
        "noise": gaussian(splits[0], (NT, S, TS), 1.0, 6.0, ((0, 8),)),
        "diagonal_tile_blocks": gaussian(splits[1], (NT, TS, TS), TS ** -0.5, 0.375, ((0, 32),)),
        "left_factors": gaussian(splits[2], (NT, NT, R, TS), (R * NT) ** -0.5, 0.046875, ((0, 8), (1, 4))),
        "right_factors": gaussian(splits[3], (NT, NT, R, TS), TS ** -0.5, 0.375, ((0, 8), (1, 4))),
        "ranks": draw_ranks(jax.random.fold_in(splits[10], 71), 0),
        "owner": draw_owner(jax.random.fold_in(splits[10], 71), 0),
        "courant_x": jnp.clip(0.05 + 0.35 * jax.random.uniform(splits[6], (GX, GY), jnp.float32) ** block_scale(splits[6], (GX, GY), ((0, 8), (1, 4)), -0.2, 0.2), 0.05, 0.4),
        "courant_number_second": jnp.clip(0.05 + 0.35 * jax.random.uniform(splits[7], (GX, GY), jnp.float32) ** block_scale(splits[7], (GX, GY), ((0, 8), (1, 4)), -0.2, 0.2), 0.05, 0.4),
        "upwind_x": place_ends(jax.random.randint(splits[8], (GX, GY), 0, 2), jax.random.fold_in(splits[8], 1), 0, 1).astype(jnp.int32),
        "upwind_y": place_ends(jax.random.randint(splits[9], (GX, GY), 0, 2), jax.random.fold_in(splits[9], 1), 0, 1).astype(jnp.int32),
    }


mixing = 0.05


def morton_table(tiles_x, tiles_y):
    bits_x = tiles_x.bit_length() - 1
    bits_y = tiles_y.bit_length() - 1
    table = np.zeros((tiles_x, tiles_y), np.int32)
    for first in range(tiles_x):
        for second in range(tiles_y):
            morton_code = 0
            position = 0
            for level in range(max(bits_x, bits_y)):
                if level < bits_y:
                    morton_code = morton_code | (((second >> level) & 1) << position)
                    position = position + 1
                if level < bits_x:
                    morton_code = morton_code | (((first >> level) & 1) << position)
                    position = position + 1
            table[first, second] = morton_code
    return table


def advance(center, low_x, high_x, low_y, high_y, courant_x, courant_number_second, upwind_x, upwind_y):
    from_x = jnp.where(upwind_x == 1, low_x, high_x)
    from_y = jnp.where(upwind_y == 1, low_y, high_y)
    return (center - courant_x * (center - from_x) - courant_number_second * (center - from_y)
            + mixing * (low_x + high_x + low_y + high_y - 4.0 * center))


def reference(noise, diagonal_tile_blocks, left_factors, right_factors, ranks, owner, courant_x, courant_number_second, upwind_x, upwind_y):
    noise_wide = noise.astype(jnp.float32)
    levels = jnp.arange(R, dtype=jnp.int32)

    def one_row(operands):
        left_row, right_row, rank_row, tile_row, diag_row = operands
        coeff = jnp.einsum('csk,crk->csr', noise_wide, right_row.astype(jnp.float32))
        keep = levels[None, None, :] < rank_row[:, None, None]
        coeff = jnp.where(keep, coeff, 0.0).astype(jnp.bfloat16)
        offdiag = jnp.einsum('csr,crk->sk', coeff.astype(jnp.float32), left_row.astype(jnp.float32))
        local_noise_tiles = lax.dynamic_index_in_dim(noise, tile_row, 0, keepdims=False)
        diagonal = jnp.dot(local_noise_tiles, jnp.tril(diag_row).T, preferred_element_type=jnp.float32)
        return offdiag + diagonal

    rowsample = lax.map(one_row, (left_factors, right_factors, ranks, owner, diagonal_tile_blocks))
    inverse_permutation = jnp.argsort(owner).astype(jnp.int32)
    sample_member = rowsample[inverse_permutation]
    table = jnp.asarray(morton_table(TX, TY)).reshape(-1)
    grid = sample_member[table].reshape(TX, TY, S, TSIDE, TSIDE)
    tracer = grid.transpose(2, 0, 3, 1, 4).reshape(S, GX, GY)
    for step_index in range(ITERS):
        tracer = advance(tracer, jnp.roll(tracer, 1, 1), jnp.roll(tracer, -1, 1),
                         jnp.roll(tracer, 1, 2), jnp.roll(tracer, -1, 2),
                         courant_x, courant_number_second, upwind_x, upwind_y)
    return tracer
```

```python
import functools

import jax
import jax.numpy as jnp
import numpy as np
from jax import lax
from jax.experimental import pallas as pl
from jax.experimental.pallas import tpu as pltpu
from jax.sharding import PartitionSpec as P

TSIDE = 16
TX = 8
TY = 16
ITERS = 4
MESH = pl.DeviceIdType.MESH
VMEM = pltpu.VMEM
SMEM = pltpu.SMEM
HALVES = 2


mixing = 0.05


def morton_table(tiles_x, tiles_y):
    bits_x = tiles_x.bit_length() - 1
    bits_y = tiles_y.bit_length() - 1
    table = np.zeros((tiles_x, tiles_y), np.int32)
    for first in range(tiles_x):
        for second in range(tiles_y):
            morton_code = 0
            position = 0
            for level in range(max(bits_x, bits_y)):
                if level < bits_y:
                    morton_code = morton_code | (second >> level & 1) << position
                    position = position + 1
                if level < bits_x:
                    morton_code = morton_code | (first >> level & 1) << position
                    position = position + 1
            table[first, second] = morton_code
    return table


def advance(
    center, low_x, high_x, low_y, high_y, courant_x, courant_number_second, upwind_x, upwind_y
):
    from_x = jnp.where(upwind_x == 1, low_x, high_x)
    from_y = jnp.where(upwind_y == 1, low_y, high_y)
    return (
        center
        - courant_x * (center - from_x)
        - courant_number_second * (center - from_y)
        + mixing * (low_x + high_x + low_y + high_y - 4.0 * center)
    )


def remote(src, dst, send_sem, recv_sem, device):
    return pltpu.make_async_remote_copy(
        src_ref=src,
        dst_ref=dst,
        send_sem=send_sem,
        recv_sem=recv_sem,
        device_id=device,
        device_id_type=MESH,
    )


def spread_kernel(
    wides,
    narrows,
    noise_ref,
    coef_ref,
    owner_ref,
    diag_ref,
    cols_ref,
    diag_out_ref,
    coefs_ref,
    picked,
    picked_in,
    noise_send,
    noise_recv,
    pass_send,
    own_sem,
    coef_send,
    coef_recv,
    own_coef_sem,
    pick_send,
    pick_recv,
):
    w = lax.axis_index("wide")
    n = lax.axis_index("narrow")
    tiles = noise_ref.shape[0]
    held = diag_ref.shape[0]
    cells = diag_ref.shape[1]
    cols = cols_ref.shape[0]
    ratio = wides // narrows
    line = wides // 2
    part = tiles // HALVES
    parity = lax.rem(w, 2)
    partner = w + 1 - 2 * parity
    place = lax.rem(w, ratio)
    is_source = w // ratio == n

    def columns(block, half):
        return cols_ref.at[pl.ds(block * tiles + half * part, part)]

    def noise_copy(step, half):
        target = parity + 2 * lax.rem(w // 2 + step, line)
        return remote(
            noise_ref.at[pl.ds(half * part, part)],
            columns(place, half),
            noise_send.at[step, half],
            noise_recv.at[place, half],
            (target, n),
        )

    own_copy = pltpu.make_async_copy(
        noise_ref, cols_ref.at[pl.ds(place * tiles, tiles)], own_sem
    )

    @pl.when(is_source)
    def _():
        for half in range(HALVES):
            for step in range(1, line):
                noise_copy(step, half).start()
        own_copy.start()

    def coef_copy(slot, step):
        target = (lax.rem(w + 1 - slot + wides, wides), lax.rem(n + step, narrows))
        return remote(
            coef_ref,
            coefs_ref.at[slot, n],
            coef_send.at[slot, step],
            coef_recv.at[slot, step],
            target,
        )

    for slot in range(3):
        for step in range(narrows):
            if slot != 1 or step != 0:
                coef_copy(slot, step).start()
    own_coef = pltpu.make_async_copy(coef_ref, coefs_ref.at[1, n], own_coef_sem)
    own_coef.start()

    def pass_copy(pair, half):
        block = 2 * pair + parity
        return remote(
            columns(block, half),
            columns(block, half),
            pass_send.at[pair, half],
            noise_recv.at[block, half],
            (partner, n),
        )

    def arrival(block, half):
        return remote(
            columns(block, half),
            columns(block, half),
            pass_send.at[0, half],
            noise_recv.at[block, half],
            (partner, n),
        )

    @pl.when(is_source)
    def _():
        own_copy.wait()

    for half in range(HALVES):
        for pair in range(ratio // 2):
            block = 2 * pair + parity

            @pl.when(w != ratio * n + block)
            def _():
                arrival(block, half).wait_recv()

            pass_copy(pair, half).start()
    for half in range(HALVES):
        for pair in range(ratio // 2):
            arrival(2 * pair + 1 - parity, half).wait_recv()

    for k in range(narrows):
        for h in range(held):
            tile = owner_ref[w * (narrows * held) + k * held + h] - n * cols
            inside = jnp.where((tile >= 0) & (tile < cols), 1.0, 0.0).astype(jnp.float32)
            block = cols_ref[jnp.clip(tile, 0, cols - 1)]
            picked[k, h] = (block.astype(jnp.float32) * inside).astype(jnp.bfloat16)

    def pick_copy(step):
        k = lax.rem(n + step, narrows)
        return remote(
            picked.at[k], picked_in.at[n], pick_send.at[step], pick_recv.at[step], (w, k)
        )

    for step in range(1, narrows):
        pick_copy(step).start()
    total = picked[n].astype(jnp.float32)
    for step in range(1, narrows):
        pick_copy(step).wait_recv()
    for step in range(1, narrows):
        total = total + picked_in[lax.rem(n - step + narrows, narrows)].astype(jnp.float32)
    row = lax.broadcasted_iota(jnp.int32, (cells, cells), 0)
    col = lax.broadcasted_iota(jnp.int32, (cells, cells), 1)
    for h in range(held):
        lower = jnp.where(col <= row, diag_ref[h].astype(jnp.float32), 0.0).astype(jnp.bfloat16)
        diag_out_ref[h] = lax.dot_general(
            total[h].astype(jnp.bfloat16),
            lower,
            (((1,), (1,)), ((), ())),
            preferred_element_type=jnp.float32,
        )

    for step in range(1, narrows):
        pick_copy(step).wait_send()
    own_coef.wait()
    for slot in range(3):
        for step in range(narrows):
            if slot != 1 or step != 0:
                coef_copy(slot, step).wait()
    for half in range(HALVES):
        for pair in range(ratio // 2):
            pass_copy(pair, half).wait_send()

    @pl.when(is_source)
    def _():
        for half in range(HALVES):
            for step in range(1, line):
                noise_copy(step, half).wait_send()


def spread(wides, narrows, noise, coef, owner, diag):
    tiles, members, cells = noise.shape
    held = diag.shape[0]
    ratio = wides // narrows
    line = wides // 2
    dma = pltpu.SemaphoreType.DMA
    vmem = pl.BlockSpec(memory_space=VMEM)
    return pl.pallas_call(
        functools.partial(spread_kernel, wides, narrows),
        name="spread",
        out_shape=(
            jax.ShapeDtypeStruct((ratio * tiles, members, cells), jnp.bfloat16),
            jax.ShapeDtypeStruct((held, members, cells), jnp.float32),
            jax.ShapeDtypeStruct((3, narrows) + coef.shape, jnp.float32),
        ),
        in_specs=[vmem, vmem, pl.BlockSpec(memory_space=SMEM), vmem],
        out_specs=(vmem, vmem, vmem),
        scratch_shapes=[
            pltpu.VMEM((narrows, held, members, cells), jnp.bfloat16),
            pltpu.VMEM((narrows, held, members, cells), jnp.bfloat16),
            dma((line, HALVES)),
            dma((ratio, HALVES)),
            dma((max(ratio // 2, 1), HALVES)),
            dma,
            dma((3, narrows)),
            dma((3, narrows)),
            dma,
            dma((narrows,)),
            dma((narrows,)),
        ],
        compiler_params=pltpu.CompilerParams(has_side_effects=True),
    )(noise, coef, owner, diag)


def rows_kernel(
    narrows, ranks_ref, cols_ref, diag_ref, left_ref, right_ref, out_ref, coeff_ref
):
    p = pl.program_id(0)
    n = lax.axis_index("narrow")
    cols = cols_ref.shape[0]
    members = cols_ref.shape[1]
    rank = right_ref.shape[2]
    held = diag_ref.shape[0]
    level = lax.broadcasted_iota(jnp.int32, (members, rank), 1)
    for c in range(cols):
        coeff = lax.dot_general(
            cols_ref[c],
            right_ref[0, c],
            (((1,), (1,)), ((), ())),
            preferred_element_type=jnp.float32,
        )
        coeff = jnp.where(level < ranks_ref[p, c], coeff, 0.0).astype(jnp.bfloat16)
        coeff_ref[:, c * rank : (c + 1) * rank] = coeff
    left = left_ref[0].reshape(cols * rank, left_ref.shape[3])
    total = jnp.dot(coeff_ref[...], left, preferred_element_type=jnp.float32)
    at = p - n * held
    mine = jnp.where((at >= 0) & (at < held), 1.0, 0.0).astype(jnp.float32)
    total = total + mine * diag_ref[jnp.clip(at, 0, held - 1)]
    group = members // narrows
    for k in range(narrows):
        out_ref[k, 0] = total[k * group : (k + 1) * group]


def row_sums(narrows, ranks, cols, diag, left, right):
    rows, count, rank, cells = left.shape
    members = cols.shape[1]
    group = members // narrows
    factor = pl.BlockSpec((1, count, rank, cells), lambda p: (p, 0, 0, 0))
    return pl.pallas_call(
        functools.partial(rows_kernel, narrows),
        name="row_sums",
        grid=(rows,),
        out_shape=jax.ShapeDtypeStruct((narrows, rows, group, cells), jnp.float32),
        in_specs=[
            pl.BlockSpec(memory_space=SMEM),
            pl.BlockSpec(cols.shape, lambda p: (0, 0, 0)),
            pl.BlockSpec(diag.shape, lambda p: (0, 0, 0)),
            factor,
            factor,
        ],
        out_specs=pl.BlockSpec((narrows, 1, group, cells), lambda p: (0, p, 0, 0)),
        scratch_shapes=[pltpu.VMEM((members, count * rank), jnp.bfloat16)],
    )(ranks, cols, diag, left, right)


def share_kernel(
    wides,
    narrows,
    part_ref,
    all_ref,
    came,
    part_send,
    part_recv,
    line_send,
    line_recv,
    pass_send,
    pass_recv,
):
    w = lax.axis_index("wide")
    n = lax.axis_index("narrow")
    size = part_ref.shape[1] // HALVES
    line = wides // 2
    parity = lax.rem(w, 2)
    partner = w + 1 - 2 * parity

    def part_copy(step, half):
        k = lax.rem(n + step, narrows)
        rows = pl.ds(half * size, size)
        return remote(
            part_ref.at[k, rows],
            came.at[n, rows],
            part_send.at[step, half],
            part_recv.at[step, half],
            (w, k),
        )

    def line_copy(step, half):
        target = parity + 2 * lax.rem(w // 2 + step, line)
        block = all_ref.at[w, pl.ds(half * size, size)]
        return remote(
            block, block, line_send.at[step, half], line_recv.at[step, half], (target, n)
        )

    def pass_copy(step, half):
        source = parity + 2 * lax.rem(w // 2 - step + line, line)
        block = all_ref.at[source, pl.ds(half * size, size)]
        return remote(
            block, block, pass_send.at[step, half], pass_recv.at[step, half], (partner, n)
        )

    for half in range(HALVES):
        for step in range(1, narrows):
            part_copy(step, half).start()
    for half in range(HALVES):
        for step in range(1, narrows):
            part_copy(step, half).wait_recv()
        rows = pl.ds(half * size, size)
        total = part_ref[n, rows]
        for step in range(1, narrows):
            total = total + came[lax.rem(n - step + narrows, narrows), rows]
        all_ref[w, rows] = total
        for step in range(1, line):
            line_copy(step, half).start()
        pass_copy(0, half).start()
    for half in range(HALVES):
        for step in range(1, line):
            line_copy(step, half).wait_recv()
            pass_copy(step, half).start()
    for half in range(HALVES):
        for step in range(line):
            pass_copy(step, half).wait()
        for step in range(1, line):
            line_copy(step, half).wait_send()
        for step in range(1, narrows):
            part_copy(step, half).wait_send()


def share(wides, narrows, part):
    line = wides // 2
    dma = pltpu.SemaphoreType.DMA
    vmem = pl.BlockSpec(memory_space=VMEM)
    return pl.pallas_call(
        functools.partial(share_kernel, wides, narrows),
        name="share",
        out_shape=jax.ShapeDtypeStruct((wides,) + part.shape[1:], jnp.float32),
        in_specs=[vmem],
        out_specs=vmem,
        scratch_shapes=[
            pltpu.VMEM(part.shape, jnp.float32),
            dma((narrows, HALVES)),
            dma((narrows, HALVES)),
            dma((line, HALVES)),
            dma((line, HALVES)),
            dma((line, HALVES)),
            dma((line, HALVES)),
        ],
        compiler_params=pltpu.CompilerParams(has_side_effects=True),
    )(part)


def exchange_kernel(narrows, in_ref, out_ref, own_sem, send, recv):
    w = lax.axis_index("wide")
    n = lax.axis_index("narrow")

    def copy(step):
        k = lax.rem(n + step, narrows)
        return remote(in_ref.at[k], out_ref.at[n], send.at[step], recv.at[step], (w, k))

    for step in range(1, narrows):
        copy(step).start()
    own = pltpu.make_async_copy(in_ref.at[n], out_ref.at[n], own_sem)
    own.start()
    own.wait()
    for step in range(1, narrows):
        copy(step).wait()


def exchange(narrows, blocks):
    dma = pltpu.SemaphoreType.DMA
    vmem = pl.BlockSpec(memory_space=VMEM)
    return pl.pallas_call(
        functools.partial(exchange_kernel, narrows),
        name="exchange",
        out_shape=jax.ShapeDtypeStruct(blocks.shape, jnp.float32),
        in_specs=[vmem],
        out_specs=vmem,
        scratch_shapes=[dma, dma((narrows,)), dma((narrows,))],
        compiler_params=pltpu.CompilerParams(has_side_effects=True),
    )(blocks)


def per_device(
    noise,
    diagonal_tile_blocks,
    left_factors,
    right_factors,
    ranks,
    owner,
    courant_x,
    courant_number_second,
    upwind_x,
    upwind_y,
):
    wides = lax.axis_size("wide")
    narrows = lax.axis_size("narrow")
    w = lax.axis_index("wide")
    block_x, block_y = courant_x.shape
    coef = jnp.stack(
        [
            courant_x,
            courant_number_second,
            upwind_x.astype(jnp.float32),
            upwind_y.astype(jnp.float32),
        ]
    )
    cols, diag, coefs = spread(wides, narrows, noise, coef, owner, diagonal_tile_blocks)
    part = row_sums(narrows, ranks, cols, diag, left_factors, right_factors)
    whole = share(wides, narrows, part)
    group, cells = whole.shape[2:]
    total_tiles = wides * whole.shape[1]
    whole = whole.reshape(total_tiles, group, cells)

    height = block_x + 2 * ITERS
    width = TY * TSIDE
    first = w * block_x - ITERS + TX * TSIDE
    first_tile = first // TSIDE
    tile_rows = (height + 2 * TSIDE - 1 - ITERS) // TSIDE
    table = jnp.asarray(morton_table(TX, TY))
    wanted = table[(first_tile + jnp.arange(tile_rows)) % TX].reshape(-1)
    matches = wanted[:, None] == owner[None, :]
    stored = jnp.sum(
        jnp.where(matches, jnp.arange(total_tiles, dtype=jnp.int32)[None, :], 0), axis=1
    )
    field = whole[stored].reshape(tile_rows, TY, group, TSIDE, TSIDE)
    field = field.transpose(2, 0, 3, 1, 4).reshape(group, tile_rows * TSIDE, width)
    field = lax.dynamic_slice_in_dim(field, first - first_tile * TSIDE, height, 1)
    coefs = coefs.transpose(2, 0, 3, 1, 4).reshape(4, 3 * block_x, width)
    coefs = coefs[:, block_x - ITERS : 2 * block_x + ITERS]
    flags_x = jnp.where(coefs[2] > 0.5, 1, 0)
    flags_y = jnp.where(coefs[3] > 0.5, 1, 0)
    for step_index in range(ITERS):
        field = advance(
            field,
            jnp.roll(field, 1, 1),
            jnp.roll(field, -1, 1),
            jnp.roll(field, 1, 2),
            jnp.roll(field, -1, 2),
            coefs[0],
            coefs[1],
            flags_x,
            flags_y,
        )
    field = field[:, ITERS : ITERS + block_x]
    field = field.reshape(group, block_x, narrows, block_y).transpose(2, 0, 1, 3)
    return exchange(narrows, field).reshape(narrows * group, block_x, block_y)


def solution(mesh):
    placed = (
        P("wide", None, None),
        P(("wide", "narrow"), None, None),
        P("wide", "narrow", None, None),
        P("wide", "narrow", None, None),
        P("wide", "narrow"),
        P(),
        P("wide", "narrow"),
        P("wide", "narrow"),
        P("wide", "narrow"),
        P("wide", "narrow"),
    )
    return jax.shard_map(
        per_device, mesh=mesh, in_specs=placed, out_specs=P(None, "wide", "narrow"), check_vma=False
    )
```
